32 devices in a mesh: dp: 2 (over y), seq: 4 (over z), chan: 4 (over x, core).
Axes of the slice: x: 2, y: 2, z: 4, core: 2. Of those that a mesh axis runs over, the one named last changes fastest.
Arguments:
- layer_input: bfloat16 [2, 512, 2560], P('dp', ('seq', 'chan')), may hold values from -6 to 6
- inner_weight: bfloat16 [2560, 2560], P(None, 'chan'), may hold values from -0.125 to 0.125
- mixer_weight: bfloat16 [2560, 256], replicated, may hold values from -0.01171875 to 0.01171875
- step_weight: bfloat16 [2560, 40], P(None, 'chan'), may hold values from -0.125 to 0.125
- conv_inner: float32 [4, 2560], P(None, 'chan'), may hold values from -3 to 3
- conv_mixer: float32 [4, 256], replicated, may hold values from -3 to 3
- step_bias: float32 [40], P('chan'), may hold values from -2 to 1
- decay_log: float32 [40], P('chan'), as said below
- skip_gain: float32 [40], P('chan'), may hold values from 0.5 to 1.5
- output_grad: bfloat16 [2, 512, 2560], P('dp', 'seq', 'chan'), may hold values from -6 to 6
Outputs:
- input_grad: bfloat16 [2, 512, 2560], P('dp', ('seq', 'chan'))
- inner_weight_grad: float32 [2560, 2560], P(('dp', 'seq'), 'chan')
- mixer_weight_grad: float32 [2560, 256], P(('dp', 'seq', 'chan'))
- step_weight_grad: float32 [2560, 40], P(('dp', 'seq'), 'chan')
The draws below stay inside these ranges and needn't reach their ends.
Inputs may be any that keep to these rules, and one draw needn't show every extreme that they name: exp(decay_log) is at least 0.2 / 512.
All inputs are finite; a program needn't handle non-finite values.
Results may differ from the reference program's by a relative error of at most 0.014.
Values may be sent and summed in bfloat16 or wider, within the bound.
A program may use at most 128 MiB of HBM per device.

```python
import math
import jax
import jax.numpy as jnp
from jax import lax

D = 2560
HEADS = 40
HDIM = 64
STATE = 128
KW = 4
BATCH = 2
LENGTH = 512
TOKENS = 1024
INNER = 2560


def draw_decay_log(key, part):
    base = jax.random.fold_in(key, 71)
    order_key, slow_key, fast_key = jax.random.split(base, 3)
    ranks = jax.random.permutation(order_key, HEADS)
    slow_count = HEADS // 2
    is_slow = ranks < slow_count
    slow_rate = jnp.exp(jax.random.uniform(slow_key, (HEADS,), jnp.float32, jnp.log(0.2), jnp.log(2.0))) / LENGTH
    fast_rate = jnp.exp(jax.random.uniform(fast_key, (HEADS,), jnp.float32, jnp.log(0.02), jnp.log(0.06)))
    return jnp.log(jnp.where(is_slow, slow_rate, fast_rate)).astype(jnp.float32)


def spiked(entries, own_key, source, target, parts, factor):
    def block_of(dim):
        return (jnp.arange(entries.shape[dim]) // (entries.shape[dim] // parts)).reshape((-1,) + (1,) * (entries.ndim - 1 - dim))

    first = jax.random.permutation(own_key, parts)[block_of(target)]
    other_side = (block_of(target) + parts // 2) % parts
    return jnp.where((block_of(source) == first) | (block_of(source) == other_side), factor * entries, entries)


def shard_levels(key, dims, cuts, least, top_value):
    gain = 1.0
    for position, shards_of in cuts:
        steps = jax.random.uniform(jax.random.fold_in(jax.random.fold_in(key, 6), position), (shards_of,), jnp.float32, least / len(cuts), top_value / len(cuts))
        gain = gain * jnp.repeat(jnp.exp(steps), dims[position] // shards_of).reshape((-1,) + (1,) * (len(dims) - 1 - position))
    return gain


def gaussian(stream_key, shape, width, most, cuts=(), held_as=jnp.bfloat16):
    values = jax.random.normal(stream_key, shape, jnp.float32) * width
    if len(cuts) > 0:
        values = shard_levels(stream_key, shape, cuts, -0.22, 0.18) * values
    return jnp.clip(values, min=-most, max=most).astype(held_as)


def noise_with(own_key, dims, width, most, cuts, heavy, kind=jnp.bfloat16):
    drawn = width * jax.random.normal(own_key, dims, jnp.float32)
    if cuts:
        drawn = drawn * shard_levels(own_key, dims, cuts, -0.22, 0.18)
    return jnp.clip(spiked(drawn, jax.random.fold_in(own_key, 3), *heavy), -most, most).astype(kind)


def setup_inputs(seed: int = 0) -> dict:
    splits = jax.random.split(jax.random.key(seed), 11)
    return {
        "layer_input": noise_with(splits[0], (BATCH, LENGTH, D), 1.0, 6.0, ((0, 2), (1, 16)), (1, 2, 16, 2.0)),
        "inner_weight": gaussian(splits[1], (D, INNER), D ** -0.5, 0.125, ((1, 4),)),
        "mixer_weight": gaussian(splits[2], (D, 2 * STATE), (0.1 / D ** 0.5), 0.01171875),
        "step_weight": gaussian(splits[3], (D, HEADS), D ** -0.5, 0.125, ((1, 4),)),
        "conv_inner": gaussian(splits[4], (KW, INNER), KW ** -0.5, 3.0, ((1, 4),), jnp.float32),
        "conv_mixer": gaussian(splits[5], (KW, 2 * STATE), KW ** -0.5, 3.0, (), jnp.float32),
        "step_bias": jnp.clip(-2.0 + 3.0 * jax.random.uniform(splits[6], (HEADS,), jnp.float32) ** shard_levels(splits[6], (HEADS,), ((0, 4),), -0.2, 0.2), -2.0, 1.0),
        "decay_log": draw_decay_log(jax.random.fold_in(splits[10], 71), 0),
        "skip_gain": jnp.clip(0.5 + 1.0 * jax.random.uniform(splits[8], (HEADS,), jnp.float32) ** shard_levels(splits[8], (HEADS,), ((0, 4),), -0.2, 0.2), 0.5, 1.5),
        "output_grad": gaussian(splits[9], (BATCH, LENGTH, INNER), 1.0, 6.0, ((0, 2), (1, 4), (2, 4))),
    }


block_tokens = 256

def conv_silu(inputs, history, kernel):
    length = inputs.shape[0]
    padded = jnp.concatenate([history, inputs], axis=0)
    summed = kernel[0][None, :] * padded[0:length]
    for offset in range(1, kernel.shape[0]):
        summed = summed + kernel[offset][None, :] * padded[offset:offset + length]
    return jax.nn.silu(summed)

def activations(inner_proj, mixer_proj, step_raw, inner_hist, mixer_hist, conv_inner, conv_mixer, step_bias, decay_log):
    length = inner_proj.shape[0]
    head_count = step_bias.shape[0]
    state_width = mixer_proj.shape[1] // 2
    inner_act = conv_silu(inner_proj, inner_hist, conv_inner).reshape(length, head_count, -1)
    mixer_act = conv_silu(mixer_proj, mixer_hist, conv_mixer)
    step_size = jax.nn.softplus(step_raw + step_bias[None, :])
    log_decay = -step_size * jnp.exp(decay_log)[None, :]
    return (inner_act, mixer_act[:, :state_width], mixer_act[:, state_width:], step_size, log_decay)

def spanned_scan(inner_act, input_mix, output_mix, step_size, log_decay, skip_gain, initial):
    length, head_count, head_dim = inner_act.shape
    block_len = min(block_tokens, length)
    blocks = length // block_len
    highest = lax.Precision.HIGHEST

    def to_blocks(values):
        return values.reshape((blocks, block_len) + values.shape[1:])

    def advance(carry_state, pieces):
        part_inner, part_input, part_output, part_step, part_decay = pieces
        cumulative = jnp.cumsum(part_decay, axis=0)
        scores = jnp.dot(part_output, part_input.T, precision=highest)
        causal = (jnp.arange(block_len)[:, None] >= jnp.arange(block_len)[None, :])[:, :, None]
        spread = cumulative[:, None, :] - cumulative[None, :, :]
        weights = jnp.where(causal, jnp.exp(jnp.where(causal, spread, 0.0)), 0.0)
        weights = weights * scores[:, :, None] * part_step[None, :, :]
        within = jnp.einsum('ijh,jhp->ihp', weights, part_inner, precision=highest)
        carried = jnp.exp(cumulative)[:, :, None] * jnp.einsum('in,hpn->ihp', part_output, carry_state, precision=highest)
        result = within + carried + skip_gain[None, :, None] * part_inner
        tail_weight = jnp.exp(cumulative[-1][None, :] - cumulative) * part_step
        update_term = jnp.einsum('jh,jhp,jn->hpn', tail_weight, part_inner, part_input, precision=highest)
        carry_state = jnp.exp(cumulative[-1])[:, None, None] * carry_state + update_term
        return (carry_state, result)
    final, results = lax.scan(jax.checkpoint(advance), initial, (to_blocks(inner_act), to_blocks(input_mix), to_blocks(output_mix), to_blocks(step_size), to_blocks(log_decay)))
    return (results.reshape(length, head_count, head_dim), final)

def contract_rows(left_rows, right_rows):
    return lax.dot_general(left_rows, right_rows, (((0,), (0,)), ((), ())), preferred_element_type=jnp.float32)

def project_back(gradient, weight):
    return lax.dot_general(gradient, weight, (((1,), (1,)), ((), ())), preferred_element_type=jnp.float32)

def reference(layer_input, inner_weight, mixer_weight, step_weight, conv_inner, conv_mixer, step_bias, decay_log, skip_gain, output_grad):
    history_len = KW - 1
    highest = lax.Precision.HIGHEST
    inner_acc = jnp.zeros((D, INNER), jnp.float32)
    mixer_acc = jnp.zeros((D, 2 * STATE), jnp.float32)
    step_acc = jnp.zeros((D, HEADS), jnp.float32)
    input_grads = []
    zero_inner = jnp.zeros((history_len, INNER), jnp.float32)
    zero_mixer = jnp.zeros((history_len, 2 * STATE), jnp.float32)
    initial = jnp.zeros((HEADS, HDIM, STATE), jnp.float32)
    for batch_row in range(BATCH):
        tokens = layer_input[batch_row]
        inner_proj = jnp.dot(tokens, inner_weight, preferred_element_type=jnp.float32).astype(jnp.bfloat16)
        mixer_proj = jnp.dot(tokens, mixer_weight, preferred_element_type=jnp.float32).astype(jnp.bfloat16)
        step_raw = jnp.dot(tokens, step_weight, preferred_element_type=jnp.float32)
        inner_wide = lax.optimization_barrier(inner_proj).astype(jnp.float32)
        mixer_wide = lax.optimization_barrier(mixer_proj).astype(jnp.float32)

        def layer(inner_in, mixer_in, step_in):
            acts = activations(inner_in, mixer_in, step_in, zero_inner, zero_mixer, conv_inner, conv_mixer, step_bias, decay_log)
            result, final = spanned_scan(acts[0], acts[1], acts[2], acts[3], acts[4], skip_gain, initial)
            return result.reshape(LENGTH, INNER)
        unused, pull = jax.vjp(layer, inner_wide, mixer_wide, step_raw)
        grad_inner, grad_mixer, grad_step = pull(output_grad[batch_row].astype(jnp.float32))
        grad_inner = grad_inner.astype(jnp.bfloat16)
        grad_step = grad_step.astype(jnp.bfloat16)
        summed = project_back(grad_inner, inner_weight) + project_back(grad_step, step_weight)
        summed = summed + lax.dot_general(grad_mixer, mixer_weight.astype(jnp.float32), (((1,), (1,)), ((), ())), precision=highest)
        input_grads.append(summed.astype(jnp.bfloat16))
        inner_acc = inner_acc + contract_rows(tokens, grad_inner)
        step_acc = step_acc + contract_rows(tokens, grad_step)
        mixer_acc = mixer_acc + lax.dot_general(tokens.astype(jnp.float32), grad_mixer, (((0,), (0,)), ((), ())), precision=highest)
    norm_factor = 1.0 / math.sqrt(TOKENS)
    return (jnp.stack(input_grads, axis=0), inner_acc * norm_factor, mixer_acc * norm_factor, step_acc * norm_factor)
```

```python
import functools
import math

import jax
import jax.numpy as jnp
from jax import lax
from jax.experimental import pallas as pl
from jax.experimental.pallas import tpu as pltpu
from jax.sharding import PartitionSpec as P

MESH = pl.DeviceIdType.MESH
HDIM = 64
PAD = 16
LANES = 128
LIMIT = 60 * 2**20
BF = jnp.bfloat16
F32 = jnp.float32
HIGH = lax.Precision.HIGHEST


def size_of(axes, sizes):
    return math.prod(sizes[a] for a in axes)


def index_of(axes, sizes):
    index = 0
    for a in axes:
        index = index * sizes[a] + lax.axis_index(a)
    return index


def coords(axes, sizes, index):
    place = {}
    for a in reversed(axes):
        place[a] = lax.rem(index, sizes[a])
        index = lax.div(index, sizes[a])
    return place


def each(n, step):
    if n <= 12:
        for d in range(1, n):
            step(d)
    else:

        def one(d, carry):
            step(d)
            return carry

        lax.fori_loop(1, n, one, 0)


def exchange_kernel(jobs, tail, plugged, sizes, *refs):
    count = len(jobs)
    extra = 1 if tail else 0
    fed = count + (1 if tail == "up" else 0)
    plug_ins, plug_outs, plug_scratch = plugged.counts if plugged else (0, 0, 0)
    cuts = (fed, plug_ins, count + extra, plug_outs, 2 * (count + extra), plug_scratch)
    groups, at = [], 0
    for cut in cuts:
        groups.append(refs[at : at + cut])
        at += cut
    ins, plug_in, outs, plug_out, sems, scratch = groups
    plug = plugged.bind(sizes, plug_in, plug_out, scratch) if plugged else None
    barrier = pltpu.get_barrier_semaphore()
    chans, seqs = sizes["chan"], sizes["seq"]
    greeted = 0
    for axes in dict.fromkeys(job[0] for job in jobs):
        n, me = size_of(axes, sizes), index_of(axes, sizes)

        def greet(d, axes=axes, n=n, me=me):
            where = coords(axes, sizes, lax.rem(me + d, n))
            pl.semaphore_signal(barrier, inc=1, device_id=where, device_id_type=MESH)

        each(n, greet)
        greeted += n - 1
    if tail:
        spot = lax.axis_index("seq")
        after, before = lax.rem(spot + 1, seqs), lax.rem(spot + seqs - 1, seqs)
        ending = lax.axis_index("chan") == chans - 1
        source = {"seq": before, "chan": jnp.int32(chans - 1)}
        signal_to(barrier, source if tail == "up" else {"seq": before})

        if tail == "up":

            @pl.when(ending)
            def _():
                for c in range(chans):
                    signal_to(barrier, {"seq": after, "chan": jnp.int32(c)})

            greeted += 1 + chans * lax.div(lax.axis_index("chan"), chans - 1)
        else:
            signal_to(barrier, {"seq": after})
            greeted += 2
    if plug:
        greeted += plug.greet(barrier)
    pl.semaphore_wait(barrier, greeted)
    if plug:
        plug.start()

    def describe(k, q, landing, signal):
        axes, mode = jobs[k]
        src = ins[k] if mode == "gather" else ins[k].at[:, q] if mode == "cross" else ins[k].at[q]
        return pltpu.make_async_remote_copy(
            src_ref=src,
            dst_ref=outs[k].at[landing],
            send_sem=sems[2 * k].at[q],
            recv_sem=sems[2 * k + 1].at[signal],
            device_id=coords(axes, sizes, q),
            device_id_type=MESH,
        )

    for k, (axes, mode) in enumerate(jobs):
        n, me = size_of(axes, sizes), index_of(axes, sizes)
        each(n, lambda d, k=k, n=n, me=me: describe(k, lax.rem(me + d, n), me, me).start())
    if tail:
        tail_out = outs[count]
        tail_in = ins[count] if tail == "up" else ins[0].at[pl.ds(ins[0].shape[0] - PAD, PAD)]
        tail_send, tail_recv = sems[2 * count], sems[2 * count + 1]

        def down(c):
            return pltpu.make_async_remote_copy(
                src_ref=tail_in if c == chans - 1 else tail_out,
                dst_ref=tail_out,
                send_sem=tail_send.at[c],
                recv_sem=tail_recv.at[0],
                device_id={"seq": after} if c == chans - 1 else {"chan": jnp.int32(c)},
                device_id_type=MESH,
            )

        def up(slot):
            return pltpu.make_async_remote_copy(
                src_ref=tail_in,
                dst_ref=tail_out.at[slot],
                send_sem=tail_send.at[0],
                recv_sem=tail_recv.at[slot],
                device_id=source,
                device_id_type=MESH,
            )

        if tail == "down":

            @pl.when(ending)
            def _():
                down(chans - 1).start()
        else:
            up(lax.axis_index("chan")).start()
    for k, (axes, mode) in enumerate(jobs):
        me = index_of(axes, sizes)
        kept = ins[k][...] if mode == "gather" else ins[k][:, me] if mode == "cross" else ins[k][me]
        outs[k][me] = kept
    if tail == "down":
        down(chans - 1).wait_recv()

        @pl.when(ending)
        def _():
            for c in range(chans - 1):
                down(c).start()

    if plug:
        plug.run()
    for k, (axes, mode) in enumerate(jobs):
        n, me = size_of(axes, sizes), index_of(axes, sizes)

        def finish(d, k=k, n=n, me=me):
            q = lax.rem(me + d, n)
            describe(k, q, q, q).wait()

        each(n, finish)
    if tail == "down":
        @pl.when(ending)
        def _():
            for c in range(chans):
                down(c).wait_send()
    if tail == "up":
        up(lax.axis_index("chan")).wait_send()

        @pl.when(ending)
        def _():
            for c in range(chans):
                up(c).wait_recv()


def signal_to(barrier, where):
    pl.semaphore_signal(barrier, inc=1, device_id=where, device_id_type=MESH)


def greet_line(barrier, n):
    me = lax.axis_index("seq")
    signal_to(barrier, {"seq": lax.rem(me + 1, n)})
    signal_to(barrier, {"seq": lax.rem(me + n - 1, n)})
    return 2


class Chain:
    counts = (3, 2, 6)
    pieces = 5

    def shapes(self, sizes, arrays):
        shape = jax.ShapeDtypeStruct(arrays[0].shape, BF)
        sems = [pltpu.SemaphoreType.DMA((self.pieces,)) for unused in range(4)]
        return [shape, shape], [pltpu.VMEM(shape.shape, BF)] * 2 + sems

    def bind(self, sizes, ins, outs, scratch):
        bound = Chain()
        bound.n, bound.ins, bound.outs, bound.scratch = sizes["seq"], ins, outs, scratch
        return bound

    def greet(self, barrier):
        return greet_line(barrier, self.n)

    def copy(self, way, piece):
        me = lax.axis_index("seq")
        rows = self.outs[0].shape[0] // self.pieces
        part = pl.ds(pl.multiple_of(piece * rows, rows), rows)
        target = lax.rem(me + 1, self.n) if way == 0 else lax.rem(me + self.n - 1, self.n)
        return pltpu.make_async_remote_copy(
            src_ref=self.scratch[way].at[part],
            dst_ref=self.outs[way].at[part],
            send_sem=self.scratch[2 + way].at[piece],
            recv_sem=self.scratch[4 + way].at[piece],
            device_id={"seq": target},
            device_id_type=MESH,
        )

    def start(self):
        me = lax.axis_index("seq")
        for way, edge in ((0, 0), (1, self.n - 1)):

            @pl.when(me == edge)
            def _(way=way):
                self.outs[way][...] = jnp.zeros(self.outs[way].shape, BF)

    def run(self):
        me = lax.axis_index("seq")
        rows = self.outs[0].shape[0] // self.pieces

        def beat(t):
            for way in (0, 1):
                place = me if way == 0 else self.n - 1 - me
                piece = t - place
                active = (piece >= 0) & (piece < self.pieces)

                @pl.when(active & (place > 0))
                def _(way=way, piece=piece):
                    self.copy(way, piece).wait_recv()

                @pl.when(active & (place < self.n - 1))
                def _(way=way, piece=piece):
                    part = pl.ds(pl.multiple_of(piece * rows, rows), rows)
                    before = self.outs[way][part, :].astype(F32)
                    term = self.ins[way][part, :].astype(F32)
                    self.scratch[way][part, :] = (self.ins[2][part, :] * before + term).astype(BF)
                    self.copy(way, piece).start()

        beat(0)
        each(self.n - 1 + self.pieces, beat)

        for way in (0, 1):

            @pl.when(me != (self.n - 1 if way == 0 else 0))
            def _(way=way):
                for piece in range(self.pieces):
                    self.copy(way, piece).wait_send()


class Grid:
    counts = (1, 1, 10)

    def shapes(self, sizes, arrays):
        d, n = sizes["dp"], sizes["seq"]
        shape = jax.ShapeDtypeStruct((d, n) + arrays[0].shape, BF)
        lengths = (n, d * n, d, d * n, n, n, d * n, d, d * n, d * n)
        return [shape], [pltpu.SemaphoreType.DMA((k,)) for k in lengths]

    def bind(self, sizes, ins, outs, scratch):
        bound = Grid()
        bound.d, bound.n = sizes["dp"], sizes["seq"]
        bound.src, bound.out, bound.sems = ins[0], outs[0], scratch
        return bound

    def greet(self, barrier):
        mine = lax.axis_index("dp")
        for e in range(1, self.d):
            signal_to(barrier, {"dp": lax.rem(mine + e, self.d)})
        return greet_line(barrier, self.n) + self.d - 1

    def copy(self, half, way, e, k, own=False, target=None):
        rows = self.src.shape[0]
        cut = (rows * 5 // 6) // 16 * 16
        part = pl.ds(0, cut) if half == 0 else pl.ds(cut, rows - cut)
        me = lax.axis_index("seq")
        slot = e * self.n + k
        if way == "cross":
            where = {"dp": lax.axis_index("dp") if target is None else target}
            recv = self.sems[1].at[slot] if half == 0 else self.sems[2].at[e]
            to = 0 if target is None else target
            send = self.sems[6].at[to * self.n + k] if half == 0 else self.sems[7].at[to]
        else:
            shift = 1 if way == "up" else self.n - 1
            where = {"seq": lax.rem(me + shift, self.n)}
            recv = self.sems[0].at[k] if half == 0 else self.sems[3].at[slot]
            ups = 4 if way == "up" else 5
            send = self.sems[ups].at[k] if half == 0 else self.sems[ups + 4].at[slot]
        src = self.src.at[part] if own else self.out.at[e, k, part]
        return pltpu.make_async_remote_copy(
            src_ref=src,
            dst_ref=self.out.at[e, k, part],
            send_sem=send,
            recv_sem=recv,
            device_id=where,
            device_id_type=MESH,
        )

    def partners(self):
        mine = lax.axis_index("dp")
        return [lax.rem(mine + e, self.d) for e in range(1, self.d)]

    def both(self, half, e, k, own=False):
        me = lax.axis_index("seq")

        @pl.when(me < self.n - 1)
        def _():
            self.copy(half, "up", e, k, own).start()

        @pl.when(me > 0)
        def _():
            self.copy(half, "down", e, k, own).start()

    def start(self):
        mine, me = lax.axis_index("dp"), lax.axis_index("seq")
        for e in self.partners():
            self.copy(1, "cross", mine, me, True, e).start()
        self.both(1, mine, me, True)
        self.both(0, mine, me, True)
        for e in self.partners():
            self.copy(0, "cross", mine, me, True, e).start()
        self.out[mine, me] = self.src[...]

    def run(self):
        mine, me, n = lax.axis_index("dp"), lax.axis_index("seq"), self.n
        others = self.partners()
        for e in others:
            self.copy(1, "cross", e, me, target=e).wait_recv()
            self.both(1, e, me)

        def hop(d):
            for way, k, there, onward in (
                ("up", me - d, me >= d, me < n - 1),
                ("down", me + d, me + d < n, me > 0),
            ):
                for e in [mine] + others:

                    @pl.when(there)
                    def _(way=way, k=k, e=e):
                        self.copy(1, way, e, k).wait_recv()

                    @pl.when(there & onward)
                    def _(way=way, k=k, e=e):
                        self.copy(1, way, e, k).start()

                @pl.when(there)
                def _(way=way, k=k):
                    self.copy(0, way, mine, k).wait_recv()

                @pl.when(there & onward)
                def _(way=way, k=k):
                    self.copy(0, way, mine, k).start()

                @pl.when(there)
                def _(way=way, k=k):
                    for e in others:
                        self.copy(0, "cross", mine, k, target=e).start()

        each(n, hop)

        def settle(k):
            for e in others:
                self.copy(0, "cross", e, k, target=e).wait_recv()
                self.copy(0, "cross", mine, k, target=e).wait_send()
            for way, sent in (("up", (k <= me) & (me < n - 1)), ("down", (k >= me) & (me > 0))):

                @pl.when(sent)
                def _(way=way, k=k):
                    self.copy(0, way, mine, k).wait_send()
                    for e in [mine] + others:
                        self.copy(1, way, e, k).wait_send()

        settle(0)
        each(n, settle)
        for e in others:
            self.copy(1, "cross", mine, me, target=e).wait_send()


def exchange(sizes, call_id, jobs, arrays, tail=None, tail_array=None, plug=None, plug_arrays=()):
    plan, out_shapes, sems = [], [], []
    for (axes, mode), array in zip(jobs, arrays):
        n = size_of(axes, sizes)
        shape = (n,) + array.shape if mode == "gather" else array.shape
        if mode == "cross":
            shape = (n, array.shape[0]) + array.shape[2:]
        plan.append((axes, mode))
        out_shapes.append(jax.ShapeDtypeStruct(shape, array.dtype))
        sems += [pltpu.SemaphoreType.DMA((n,)), pltpu.SemaphoreType.DMA((n,))]
    arrays = list(arrays)
    if tail:
        if tail == "up":
            arrays.append(tail_array)
            shape = (sizes["chan"],) + tail_array.shape
        else:
            shape = (PAD,) + arrays[0].shape[1:]
        out_shapes.append(jax.ShapeDtypeStruct(shape, arrays[0].dtype))
        sems += [pltpu.SemaphoreType.DMA((sizes["chan"],)), pltpu.SemaphoreType.DMA((sizes["chan"],))]
    if plug:
        arrays += plug_arrays
        plug_shapes, plug_scratch = plug.shapes(sizes, plug_arrays)
        out_shapes += plug_shapes
        sems += plug_scratch
    vmem = pl.BlockSpec(memory_space=pltpu.VMEM)
    return pl.pallas_call(
        functools.partial(exchange_kernel, tuple(plan), tail, plug, sizes),
        out_shape=out_shapes,
        in_specs=[vmem] * len(arrays),
        out_specs=[vmem] * len(out_shapes),
        scratch_shapes=sems,
        compiler_params=pltpu.CompilerParams(
            collective_id=call_id, has_side_effects=True, vmem_limit_bytes=LIMIT
        ),
        name=f"exchange_{call_id}",
    )(*arrays)


def mm(a, b, da, db):
    return lax.dot_general(
        a.astype(BF), b.astype(BF), (((da,), (db,)), ((), ())), preferred_element_type=F32
    )


def exact(a, b, da=1, db=0):
    return lax.dot_general(
        a, b, (((da,), (db,)), ((), ())), precision=HIGH, preferred_element_type=F32
    )


def softplus(v):
    return jnp.maximum(v, 0.0) + jnp.log1p(jnp.exp(-jnp.abs(v)))


def head_mask(width, heads_first):
    shape = (LANES, width) if heads_first else (width, LANES)
    head = lax.broadcasted_iota(jnp.int32, shape, 0 if heads_first else 1)
    column = lax.broadcasted_iota(jnp.int32, shape, 1 if heads_first else 0)
    return (column // HDIM == head).astype(F32)


def decays(raw, bias, decay_log):
    length = raw.shape[0]
    step = softplus(raw + bias)
    rate = jnp.exp(decay_log)
    row = lax.broadcasted_iota(jnp.int32, (length, length), 0)
    col = lax.broadcasted_iota(jnp.int32, (length, length), 1)
    lower = (row >= col).astype(F32)
    cumulative = exact(lower, -step * rate)
    return step, rate, cumulative, row, col, lower


def forward_kernel(
    inner_ref, mixer_ref, raw_ref, conv_inner_ref, conv_mixer_ref, bias_ref, log_ref, grad_ref,
    summed_inner_ref, summed_mixer_ref, state_ref, back_ref, decay_ref, wide_inner, wide_mixer,
):
    length = raw_ref.shape[0]
    width = conv_inner_ref.shape[1]
    taps = conv_inner_ref.shape[0]
    wide_inner[...] = inner_ref[...].astype(F32)
    wide_mixer[...] = mixer_ref[...].astype(F32)
    first = PAD - (taps - 1)

    def convolved(wide, kernel):
        total = kernel[0:1, :] * wide[pl.ds(first, length), :]
        for k in range(1, taps):
            total = total + kernel[k : k + 1, :] * wide[pl.ds(first + k, length), :]
        return total

    inner = convolved(wide_inner, conv_inner_ref)
    mixer = convolved(wide_mixer, conv_mixer_ref)
    summed_inner_ref[...] = inner
    summed_mixer_ref[...] = mixer
    act = inner * jax.nn.sigmoid(inner)
    mix = mixer * jax.nn.sigmoid(mixer)
    half = mix.shape[1] // 2
    step, rate, cumulative, row, col, lower = decays(raw_ref[...], bias_ref[...], log_ref[...])
    last = cumulative[length - 1 : length, :]
    spread = head_mask(width, True)
    tail = exact(jnp.exp(last - cumulative) * step, spread)
    grown = exact(jnp.exp(cumulative), spread)
    upstream = grad_ref[...].astype(F32)
    state_ref[...] = mm(act * tail, mix[:, :half], 0, 0).astype(BF)
    back_ref[...] = mm(grown * upstream, mix[:, half:], 0, 0).astype(BF)
    row_decay = jnp.sum(head_mask(width, False) * jnp.exp(last), axis=1, keepdims=True)
    decay_ref[...] = jnp.broadcast_to(row_decay, decay_ref.shape)


def backward_kernel(
    heads, inner_ref, mixer_ref, raw_ref, conv_inner_ref, conv_mixer_ref, bias_ref, log_ref,
    skip_ref, grad_ref, start_ref, end_ref,
    out_ref, step_ref, z_ref, y_ref, pad_inner, pad_mixer,
):
    length = raw_ref.shape[0]
    width = conv_inner_ref.shape[1]
    taps = conv_inner_ref.shape[0]
    spread = head_mask(width, True)
    spread_down = head_mask(width, False)
    start, end = start_ref[...].astype(F32), end_ref[...].astype(F32)
    inner, mixer = inner_ref[...], mixer_ref[...]
    inner_gate, mixer_gate = jax.nn.sigmoid(inner), jax.nn.sigmoid(mixer)
    act, mix = inner * inner_gate, mixer * mixer_gate
    half = mix.shape[1] // 2
    into, out_of = mix[:, :half], mix[:, half:]
    raw = raw_ref[...]
    step, rate, cumulative, row, col, lower = decays(raw, bias_ref[...], log_ref[...])
    last = cumulative[length - 1 : length, :]
    step_wide = exact(step, spread)
    grown = exact(jnp.exp(cumulative), spread)
    fading = exact(jnp.exp(last - cumulative), spread)
    upstream_low = grad_ref[...]
    upstream = upstream_low.astype(F32)
    stepped_low = (act * step_wide).astype(BF)
    stepped = stepped_low.astype(F32)
    scores = mm(out_of, into, 1, 1)
    causal = row >= col
    across = cumulative.T
    score_grad = jnp.zeros((length, length), F32)
    for h in range(heads):
        cols = slice(h * HDIM, (h + 1) * HDIM)
        gap = cumulative[:, h : h + 1] - across[h : h + 1, :]
        decay = jnp.where(causal, jnp.exp(jnp.where(causal, gap, 0.0)), 0.0)
        weights = (decay * scores).astype(BF)
        grad_h, step_h = upstream_low[:, cols], stepped_low[:, cols]
        score_grad = score_grad + decay * mm(grad_h, step_h, 1, 1)
        z_ref[:, cols] = mm(weights, grad_h, 0, 0)
        y_ref[:, cols] = mm(weights, step_h, 1, 0)
    z = z_ref[...]
    carried = grown * mm(out_of, start, 1, 1)
    ending = fading * mm(into, end, 1, 1)
    act_grad = step_wide * (z + ending) + exact(skip_ref[...], spread)[0:1, :] * upstream
    to_heads = functools.partial(exact, b=spread, da=1, db=1)
    step_grad = to_heads(act * (z + ending))
    tail_term = to_heads(stepped * ending)
    sum_grad = to_heads(upstream * (y_ref[...] + carried) - stepped * z) - tail_term
    held = jnp.sum(start * end, axis=1, keepdims=True)
    overall = jnp.sum(tail_term, axis=0, keepdims=True) + jnp.exp(last) * jnp.sum(
        spread_down * held, axis=0, keepdims=True
    )
    decay_grad = exact(lower, sum_grad, 0, 0) + overall
    step_grad = (step_grad - rate * decay_grad) * jax.nn.sigmoid(raw + bias_ref[...])
    out_grad = mm(score_grad, into, 1, 0) + mm(grown * upstream, start, 1, 0)
    into_grad = mm(score_grad, out_of, 0, 0) + mm(fading * stepped, end, 1, 0)
    inner_slope = inner_gate * (1.0 + inner * (1.0 - inner_gate))
    mixer_slope = mixer_gate * (1.0 + mixer * (1.0 - mixer_gate))
    for pad in (pad_inner, pad_mixer):
        pad[0:PAD, :] = jnp.zeros((PAD, pad.shape[1]), F32)
        pad[PAD + length :, :] = jnp.zeros((PAD, pad.shape[1]), F32)
    pad_inner[PAD : PAD + length, :] = act_grad * inner_slope
    pad_mixer[PAD : PAD + length, :half] = into_grad * mixer_slope[:, :half]
    pad_mixer[PAD : PAD + length, half:] = out_grad * mixer_slope[:, half:]

    def spread_back(pad, kernel):
        total = None
        for k in range(taps):
            term = kernel[k : k + 1, :] * pad[pl.ds(taps - 1 - k, PAD + length), :]
            total = term if total is None else total + term
        return total.astype(BF)

    mixer_end = width + 2 * half
    inner_back = spread_back(pad_inner, conv_inner_ref)
    out_ref[:, 0:width] = inner_back
    out_ref[0:PAD, 0:LANES] = (inner_back[0:PAD, 0:LANES].astype(F32) + step_grad.T[0:PAD, :]).astype(BF)
    out_ref[:, width:mixer_end] = spread_back(pad_mixer, conv_mixer_ref)
    step_ref[...] = step_grad.astype(BF)


def local_call(kernel, out_shapes, scratch, name, *arrays):
    vmem = pl.BlockSpec(memory_space=pltpu.VMEM)
    return pl.pallas_call(
        kernel,
        out_shape=out_shapes,
        in_specs=[vmem] * len(arrays),
        out_specs=jax.tree.map(lambda unused: vmem, out_shapes),
        scratch_shapes=scratch,
        compiler_params=pltpu.CompilerParams(vmem_limit_bytes=LIMIT),
        name=name,
    )(*arrays)


def rows_dot(gradient, weight):
    return lax.dot_general(
        gradient, weight, (((1,), (1,)), ((), ())), preferred_element_type=F32
    )


def body(
    sizes,
    layer_input,
    inner_weight,
    mixer_weight,
    step_weight,
    conv_inner,
    conv_mixer,
    step_bias,
    decay_log,
    skip_gain,
    output_grad,
):
    own = layer_input[0]
    rows, model = own.shape
    chans, seqs, dps = sizes["chan"], sizes["seq"], sizes["dp"]
    groups = dps * seqs
    length = rows * chans
    width = inner_weight.shape[1]
    mixed = mixer_weight.shape[1]
    heads = step_bias.shape[0]
    blocks = own.reshape(rows, dps, seqs, model // groups).transpose(1, 2, 0, 3)
    gathered, own_columns, history = exchange(
        sizes, 0, ((("chan",), "gather"), (("dp",), "swap")), (own, blocks), "down"
    )
    history = jnp.where(lax.axis_index("seq") > 0, history, jnp.zeros_like(history))
    tokens = jnp.concatenate([history, gathered.reshape(length, model)], axis=0)
    lane_pad = ((0, 0), (0, LANES - heads))
    step_wide = jnp.pad(step_weight, lane_pad)
    inner_proj = jnp.dot(tokens, inner_weight, preferred_element_type=F32).astype(BF)
    mixer_proj = jnp.dot(tokens, mixer_weight, preferred_element_type=F32).astype(BF)
    step_raw = jnp.dot(tokens[PAD:], step_wide, preferred_element_type=F32)
    vectors = jnp.pad(jnp.stack((step_bias, decay_log, skip_gain)), ((0, 5), lane_pad[1]))
    bias, rates, skips = vectors[0:1], vectors[1:2], vectors[2:3]
    upstream = output_grad[0]
    inner_sum, mixer_sum, state, back_state, decay = local_call(
        forward_kernel,
        (
            jax.ShapeDtypeStruct((length, width), F32),
            jax.ShapeDtypeStruct((length, mixed), F32),
            jax.ShapeDtypeStruct((width, mixed // 2), BF),
            jax.ShapeDtypeStruct((width, mixed // 2), BF),
            jax.ShapeDtypeStruct((width, mixed // 2), F32),
        ),
        [pltpu.VMEM((PAD + length, width), F32), pltpu.VMEM((PAD + length, mixed), F32)],
        "forward",
        inner_proj, mixer_proj, step_raw, conv_inner, conv_mixer, bias, rates, upstream,
    )
    columns, start, end = exchange(
        sizes,
        1,
        ((("seq",), "cross"),),
        (own_columns,),
        plug=Chain(),
        plug_arrays=(state, back_state, decay),
    )
    assert length == LANES and heads + conv_inner.shape[0] - 1 <= PAD
    grads, step_grads = local_call(
        functools.partial(backward_kernel, heads),
        (
            jax.ShapeDtypeStruct((PAD + length, width + mixed), BF),
            jax.ShapeDtypeStruct((length, LANES), BF),
        ),
        [
            pltpu.VMEM((length, width), F32),
            pltpu.VMEM((length, width), F32),
            pltpu.VMEM((2 * PAD + length, width), F32),
            pltpu.VMEM((2 * PAD + length, mixed), F32),
        ],
        "backward",
        inner_sum, mixer_sum, step_raw, conv_inner, conv_mixer, bias, rates,
        jnp.broadcast_to(skips, (8, LANES)), upstream, start, end,
    )
    partial = rows_dot(grads[:, :width], inner_weight)
    partial = partial + rows_dot(grads[:, width:], mixer_weight)
    main_part = (partial[PAD:] + rows_dot(step_grads, step_wide)).astype(BF)
    tail_part = partial[:PAD].astype(BF)
    parts = main_part.reshape(chans, rows, model)
    parts, columns, tails, all_grads = exchange(
        sizes,
        2,
        ((("chan",), "swap"), (("chan",), "gather")),
        (parts, columns),
        "up",
        tail_part,
        Grid(),
        (grads,),
    )
    total = jnp.sum(parts.astype(F32), axis=0)
    reached = (lax.axis_index("chan") == chans - 1) & (lax.axis_index("seq") < seqs - 1)
    live = lax.broadcasted_iota(jnp.int32, (PAD, 1), 0) > PAD - conv_inner.shape[0]
    tail_sum = jnp.where(reached & live, jnp.sum(tails.astype(F32), axis=0), 0.0)
    total = jnp.concatenate([total[: rows - PAD], total[rows - PAD :] + tail_sum], axis=0)
    input_grad = total.astype(BF)

    split = all_grads
    main, early = split[:, :, PAD:], jnp.where(live, split[:, :, :PAD], 0)
    steps = split[:, :, :heads, :LANES].transpose(0, 1, 3, 2).reshape(groups * length, heads)
    early = jnp.concatenate([early[:, 1:], jnp.zeros_like(early[:, :1])], axis=1)
    final = (main[:, :, length - PAD :].astype(F32) + early.astype(F32)).astype(BF)
    main = jnp.concatenate([main[:, :, : length - PAD], final], axis=2)
    main = main.reshape(groups * length, -1)
    columns = columns.transpose(2, 1, 0, 3, 4).reshape(groups * length, model // groups)
    norm_factor = 1.0 / math.sqrt(groups * length)

    def term(right):
        dims = (((0,), (0,)), ((), ()))
        return norm_factor * lax.dot_general(columns, right, dims, preferred_element_type=F32)

    mixer_terms = term(main[:, width:]).reshape(chans, -1, mixed)
    (mixer_parts,) = exchange(sizes, 3, ((("chan",), "swap"),), (mixer_terms,))
    mixer_weight_grad = jnp.sum(mixer_parts, axis=0)
    return (
        input_grad[None],
        term(main[:, :width]),
        mixer_weight_grad,
        term(steps),
    )


def solution(mesh):
    sizes = dict(mesh.shape)
    in_specs = (
        P("dp", ("seq", "chan"), None),
        P(None, "chan"),
        P(),
        P(None, "chan"),
        P(None, "chan"),
        P(),
        P("chan"),
        P("chan"),
        P("chan"),
        P("dp", "seq", "chan"),
    )
    out_specs = (
        P("dp", ("seq", "chan"), None),
        P(("dp", "seq"), "chan"),
        P(("dp", "seq", "chan"), None),
        P(("dp", "seq"), "chan"),
    )
    return jax.shard_map(
        functools.partial(body, sizes),
        mesh=mesh,
        in_specs=in_specs,
        out_specs=out_specs,
        check_vma=False,
    )
```
